1024 devices in a mesh: gx: 16 (over y, x), gy: 64 (over z, core).
Axes of the slice: x: 4, y: 4, z: 32, core: 2. Of those that a mesh axis runs over, the one named last changes fastest.
Arguments:
- chemical_concentration: float32 [53, 512, 8192], P(None, 'gx', 'gy'), may hold values from 0.01 to 1
- thermal_scaled: float32 [512, 8192], P('gx', 'gy'), may hold values from 1 to 2.5
- tentative_flow_spread: float32 [512, 8192], P('gx', 'gy'), may hold values from -6 to 6
- substep_numbers: int32 [16, 1024], P('gx', 'gy'), may hold values from 1 to 4, as said below
- patch_holder_lookup: int32 [16, 1024], P('gx', 'gy'), may hold values from 0 to 15, as said below
- consumed_weighting: float32 [325, 53], replicated, may hold values from -0.875 to 0.875
- molar_coefficient: float32 [325, 53], replicated, may hold values from -0.15625 to 0.15625
- frequency_factor_log: float32 [325], replicated, may hold values from -1 to 1
- arrhenius_energy: float32 [325], replicated, may hold values from 0.5 to 3
- enthalpy_released: float32 [325], replicated, may hold values from -0.3125 to 0.3125
Outputs:
- chemicals_after_window: float32 [53, 512, 8192], P(None, 'gx', 'gy')
- thermal_after_window: float32 [512, 8192], P('gx', 'gy')
- scalar_potential_field: float32 [512, 8192], P('gx', 'gy')
- holder_energy_burden: float32 [16, 64], P('gx', 'gy')
The draws below stay inside these ranges and needn't reach their ends.
Inputs may be any that keep to these rules, and one draw needn't show every extreme that they name: `substep_numbers`: every block has 4 on some tile. `patch_holder_lookup`: in each block's 16 entries every owner 0 to 15 appears exactly 1 times.
All inputs are finite; a program needn't handle non-finite values.
Results may differ from the reference program's by a relative error of at most 0.0003.
Values sent between devices are 32-bit elements; how exact they have to be, the bound alone decides.
A program may use at most 32 MiB of HBM per device.

```python
import math
import jax
import jax.numpy as jnp
from jax import lax

NS = 53
NR = 325
CHIP_SPAN_ALPHA = 32
CHIP_SPAN_BETA = 128
MAXSUB = 4
LEVELS = 3
SWEEPS = 2
COARSE = 4
CHIP_PATCHES = 16
PATCH_VOLUMES = 256
MESH_SPAN_ALPHA = 512
MESH_SPAN_BETA = 8192
N_GX = 16
N_GY = 64


def tile_counts(key):
    heavy_key = jax.random.fold_in(key, 11)
    raw_key = jax.random.fold_in(key, 12)
    heaviness = jax.random.randint(heavy_key, (N_GX, N_GY, 1), 0, MAXSUB)
    raw = jax.random.randint(raw_key, (N_GX, N_GY, CHIP_PATCHES), 0, MAXSUB - 1)
    tallies = jnp.where(raw < heaviness, MAXSUB, 1)
    tallies = tallies.at[:, :, 0].set(MAXSUB)
    return tallies.astype(jnp.int32)


def draw_substep_numbers(key, part):
    tallies = tile_counts(key)
    return tallies.reshape(N_GX, N_GY * CHIP_PATCHES).astype(jnp.int32)


def draw_patch_holder_lookup(key, part):
    tallies = tile_counts(key)
    base = jax.random.fold_in(key, 21)
    keys = jax.random.split(base, N_GX * N_GY)
    breaker = jax.vmap(lambda single: jax.random.permutation(single, CHIP_PATCHES))(keys)
    breaker = breaker.reshape(N_GX, N_GY, CHIP_PATCHES).astype(jnp.int32)
    score = tallies * CHIP_PATCHES + breaker
    order = jnp.argsort(-score, axis=-1, stable=True)
    ranks = jnp.argsort(order, axis=-1, stable=True).astype(jnp.int32)
    row_index = jnp.arange(N_GX, dtype=jnp.int32)[:, None, None]
    owners = (ranks + row_index) % N_GX
    return owners.reshape(N_GX, N_GY * CHIP_PATCHES).astype(jnp.int32)


def steps_of(key, shape, cuts, low, top_value):
    gain = 1.0
    for dim, blocks in cuts:
        heights = jax.random.uniform(jax.random.fold_in(jax.random.fold_in(key, 6), dim), (blocks,), jnp.float32, low / len(cuts), top_value / len(cuts))
        gain = gain * jnp.repeat(jnp.exp(heights), shape[dim] // blocks).reshape((-1,) + (1,) * (len(shape) - 1 - dim))
    return gain


def scatter_about(stream_key, dims, spread, most, pieces=(), kind=jnp.bfloat16):
    array = jax.random.normal(stream_key, dims, jnp.float32) * spread
    if len(pieces) > 0:
        array = steps_of(stream_key, dims, pieces, -0.22, 0.18) * array
    return jnp.clip(array, min=-most, max=most).astype(kind)


def setup_inputs(seed: int = 0) -> dict:
    streams_of = jax.random.split(jax.random.key(seed), 11)
    return {
        "chemical_concentration": jnp.clip(jnp.exp(math.log(1.0) - 4.6051702 * jax.random.uniform(streams_of[0], (NS, MESH_SPAN_ALPHA, MESH_SPAN_BETA), jnp.float32) ** steps_of(streams_of[0], (NS, MESH_SPAN_ALPHA, MESH_SPAN_BETA), ((1, 16), (2, 64)), -0.2, 0.2)), 0.01, 1.0),
        "thermal_scaled": jnp.clip(1.0 + 1.5 * jax.random.uniform(streams_of[1], (MESH_SPAN_ALPHA, MESH_SPAN_BETA), jnp.float32) ** steps_of(streams_of[1], (MESH_SPAN_ALPHA, MESH_SPAN_BETA), ((0, 16), (1, 64)), -0.2, 0.2), 1.0, 2.5),
        "tentative_flow_spread": scatter_about(streams_of[2], (MESH_SPAN_ALPHA, MESH_SPAN_BETA), 1.0, 6.0, ((0, 16), (1, 64)), jnp.float32),
        "substep_numbers": draw_substep_numbers(jax.random.fold_in(streams_of[10], 71), 0),
        "patch_holder_lookup": draw_patch_holder_lookup(jax.random.fold_in(streams_of[10], 71), 0),
        "consumed_weighting": scatter_about(streams_of[5], (NR, NS), NS ** -0.5, 0.875, (), jnp.float32),
        "molar_coefficient": scatter_about(streams_of[6], (NR, NS), (4 * NR) ** -0.5, 0.15625, (), jnp.float32),
        "frequency_factor_log": jnp.clip(jax.random.uniform(streams_of[7], (NR,), jnp.float32, -1.0, 1.0), -1.0, 1.0),
        "arrhenius_energy": jnp.clip(jax.random.uniform(streams_of[8], (NR,), jnp.float32, 0.5, 3.0), 0.5, 3.0),
        "enthalpy_released": scatter_about(streams_of[9], (NR,), NR ** -0.5, 0.3125, (), jnp.float32),
    }


step_time = 0.4
relax = 0.8
high = lax.Precision.HIGHEST


def advance_chemistry(spec_in, temp_in, tallies, consumed_weighting, molar_coefficient, frequency_factor_log, arrhenius_energy, enthalpy_released, bound):
    width = step_time / tallies.astype(jnp.float32)
    heat_in = jnp.zeros_like(temp_in)

    def sweep(turn, carry):
        spec_now, temp_now, heat_now = carry
        delta = jnp.where(turn < tallies, width, 0.0)
        progress = jnp.einsum('rs,sbc->rbc', consumed_weighting, spec_now, precision=high)
        rates = jnp.exp(frequency_factor_log[:, None, None] - arrhenius_energy[:, None, None] / (1.0 + jnp.abs(temp_now))[None])
        flux = rates * progress
        change = jnp.einsum('rs,rbc->sbc', molar_coefficient, flux, precision=high)
        release = jnp.einsum('r,rbc->bc', enthalpy_released, flux, precision=high)
        return (spec_now + delta[None, :, None] * change, temp_now + delta[:, None] * release, heat_now + delta[:, None] * release)

    return lax.fori_loop(0, bound, sweep, (spec_in, temp_in, heat_in))


def gather_patches(grid):
    lead = grid.shape[:-2]
    depth = len(lead)
    split = grid.reshape(lead + (N_GX, CHIP_SPAN_ALPHA, N_GY, CHIP_SPAN_BETA))
    split = jnp.moveaxis(split, (depth, depth + 2), (0, 1))
    return split.reshape((N_GX * N_GY,) + lead + (CHIP_SPAN_ALPHA * CHIP_SPAN_BETA,))


def scatter_patches(blocks, lead):
    depth = len(lead)
    joined = blocks.reshape((N_GX, N_GY) + lead + (CHIP_SPAN_ALPHA, CHIP_SPAN_BETA))
    joined = jnp.moveaxis(joined, (0, 1), (depth, depth + 2))
    return joined.reshape(lead + (N_GX * CHIP_SPAN_ALPHA, N_GY * CHIP_SPAN_BETA))


def beside_all(field):
    padded = jnp.pad(field, 1)
    return padded[2:, 1:-1] + padded[:-2, 1:-1] + padded[1:-1, 2:] + padded[1:-1, :-2]


def smooth(field, rhs, scale):
    return field + relax * (scale * rhs - 4.0 * field + beside_all(field)) / 4.0


def vcycle(rhs, level):
    scale = 4.0 ** level
    field = jnp.zeros_like(rhs)
    if level == LEVELS - 1:
        for turn in range(COARSE):
            field = smooth(field, rhs, scale)
        return field
    for turn in range(SWEEPS):
        field = smooth(field, rhs, scale)
    resid = rhs - (4.0 * field - beside_all(field)) / scale
    leading_span, trailing_span = resid.shape
    coarse = resid.reshape(leading_span // 2, 2, trailing_span // 2, 2).mean(axis=(1, 3))
    correction = vcycle(coarse, level + 1)
    field = field + jnp.repeat(jnp.repeat(correction, 2, axis=0), 2, axis=1)
    for turn in range(SWEEPS):
        field = smooth(field, rhs, scale)
    return field


def reference(chemical_concentration, thermal_scaled, tentative_flow_spread, substep_numbers, patch_holder_lookup, consumed_weighting, molar_coefficient, frequency_factor_log, arrhenius_energy, enthalpy_released):
    chip_total = N_GX * N_GY
    chemical_patches = gather_patches(chemical_concentration).reshape(chip_total, NS, CHIP_PATCHES, PATCH_VOLUMES)
    thermal_patches = gather_patches(thermal_scaled).reshape(chip_total, CHIP_PATCHES, PATCH_VOLUMES)
    tallies = substep_numbers.reshape(N_GX, N_GY, CHIP_PATCHES).reshape(chip_total, CHIP_PATCHES)

    def single_patch(packed):
        spec_one, temp_one, count_one = packed
        return advance_chemistry(spec_one, temp_one, count_one, consumed_weighting, molar_coefficient, frequency_factor_log, arrhenius_energy, enthalpy_released, MAXSUB)

    updated_chemicals, thermal_following, thermal_release = lax.map(single_patch, (chemical_patches, thermal_patches, tallies))
    tile_sums = jnp.sum(thermal_release * thermal_release, axis=-1).reshape(N_GX, N_GY, CHIP_PATCHES)
    owners = patch_holder_lookup.reshape(N_GX, N_GY, CHIP_PATCHES)
    onehot = (owners[..., None] == jnp.arange(N_GX, dtype=jnp.int32)).astype(jnp.float32)
    holder_energy_burden = jnp.einsum('xyt,xyto->oy', tile_sums, onehot, precision=high) / (CHIP_SPAN_ALPHA * CHIP_SPAN_BETA)
    chemicals_after_window = scatter_patches(updated_chemicals.reshape(chip_total, NS, CHIP_SPAN_ALPHA * CHIP_SPAN_BETA), (NS,))
    thermal_after_window = scatter_patches(thermal_following.reshape(chip_total, CHIP_SPAN_ALPHA * CHIP_SPAN_BETA), ())
    heat_grid = scatter_patches(thermal_release.reshape(chip_total, CHIP_SPAN_ALPHA * CHIP_SPAN_BETA), ())
    scalar_potential_field = vcycle(tentative_flow_spread + heat_grid, 0)
    return chemicals_after_window, thermal_after_window, scalar_potential_field, holder_energy_burden
```

```python
import functools

import jax
import jax.numpy as jnp
from jax import lax
from jax.experimental import pallas as pl
from jax.experimental.pallas import tpu as pltpu
from jax.sharding import PartitionSpec as P

NS = 53
NR = 325
MAXSUB = 4
TILES = 16
ROWS = 32
LANES = 128
STATE = 64
REACT = 336
TEMP_ROW = 53
HEAT_ROW = 54
GROUPS = 4
GROUP_ROWS = ROWS // GROUPS
step_time = 0.4
MESH = pl.DeviceIdType.MESH


def halves(x):
    top = x.astype(jnp.bfloat16)
    rest = (x - top.astype(jnp.float32)).astype(jnp.bfloat16)
    return top, rest


def chemistry_kernel(
    counts,
    owners,
    chem_hbm,
    temp_ref,
    flow_ref,
    weight_ref,
    molar_ref,
    factor_ref,
    energy_ref,
    release_ref,
    chem_out,
    temp_out,
    rhs_ref,
    share_ref,
    chem_buf,
    out_buf,
    state,
    wide,
    energy_cols,
    first,
    second,
    third,
    pad,
    in_sem,
    out_sem,
):
    def fetch(g):
        return pltpu.make_async_copy(
            chem_hbm.at[:, pl.ds(g * GROUP_ROWS, GROUP_ROWS), :], chem_buf.at[g], in_sem.at[g]
        )

    def emit(g):
        return pltpu.make_async_copy(
            out_buf.at[g], chem_out.at[:, pl.ds(g * GROUP_ROWS, GROUP_ROWS), :], out_sem.at[g]
        )

    for g in range(GROUPS):
        fetch(g).start()

    wide[...] = jnp.zeros_like(wide)
    wide[0:NS, 0:NR] = weight_ref[...] * jnp.exp(factor_ref[...].reshape(1, NR))
    whole = wide[0:STATE, :]
    top = whole.astype(jnp.bfloat16).astype(jnp.float32)
    both = jnp.concatenate([top, whole - top], axis=0).T[0:REACT].astype(jnp.bfloat16)
    first[:, 0:128] = both
    first[:, 128:256] = both

    pad[...] = jnp.zeros_like(pad)
    pad[0:1, 0:NR] = energy_ref[...].reshape(1, NR) * -1.4426950408889634
    columns = jnp.broadcast_to(pad[...], (LANES, 384)).T[0:REACT]
    energy_cols[:, 0:128] = columns
    energy_cols[:, 128:256] = columns

    wide[0:NS, 0:NR] = molar_ref[...]
    wide[TEMP_ROW : TEMP_ROW + 1, 0:NR] = release_ref[...].reshape(1, NR)
    wide[HEAT_ROW : HEAT_ROW + 1, 0:NR] = release_ref[...].reshape(1, NR)
    whole = wide[0:56, :]
    top = whole.astype(jnp.bfloat16).astype(jnp.float32)
    hi = jnp.concatenate([top, whole - top], axis=0).astype(jnp.bfloat16)
    second[:, 0:384] = hi
    third[...] = wide[...].astype(jnp.bfloat16)

    for g in range(GROUPS):
        fetch(g).wait()
        rows = chem_buf.at[g].reshape(NS * GROUP_ROWS, LANES)
        for j in range(GROUP_ROWS):
            r = g * GROUP_ROWS + j
            lanes = pl.ds(r * LANES, LANES)
            state[0:NS, lanes] = rows[pl.ds(j, NS, stride=GROUP_ROWS), :]
    state[NS:STATE, :] = jnp.zeros((STATE - NS, ROWS * LANES), jnp.float32)
    for r in range(ROWS):
        state[TEMP_ROW : TEMP_ROW + 1, r * LANES : (r + 1) * LANES] = temp_ref[r : r + 1, :]

    def turn_body(turn, carry):
        def before(t):
            now = state[:, t * 256 : (t + 1) * 256]
            top, rest = halves(now)
            taken = jnp.concatenate([top, top, rest, rest], axis=0)
            return jnp.dot(first[...], taken, preferred_element_type=jnp.float32)

        def after(t, progress):
            cells = pl.ds(t * 256, 256)
            inverse = 1.0 / (1.0 + jnp.abs(state[TEMP_ROW : TEMP_ROW + 1, cells]))
            flux = jnp.exp2(energy_cols[...] * inverse) * progress
            top, rest = halves(flux)
            made = jnp.dot(second[:, 0:REACT], top, preferred_element_type=jnp.float32)
            more = jnp.dot(third[:, 0:REACT], rest, preferred_element_type=jnp.float32)
            change = made[0:56] + made[56:112] + more[0:56]
            count = jnp.full((1, 256), counts[0, t], jnp.int32)
            width = step_time / count.astype(jnp.float32)
            delta = jnp.where(turn < count, width, 0.0)
            state[0:56, cells] += delta * change

        ahead = before(0)
        for t in range(TILES):
            progress = ahead
            if t + 1 < TILES:
                ahead = before(t + 1)
            after(t, progress)
        return carry

    lax.fori_loop(0, MAXSUB, turn_body, 0)

    for g in range(GROUPS):
        rows = out_buf.at[g].reshape(NS * GROUP_ROWS, LANES)
        for j in range(GROUP_ROWS):
            r = g * GROUP_ROWS + j
            rows[pl.ds(j, NS, stride=GROUP_ROWS), :] = state[0:NS, pl.ds(r * LANES, LANES)]
        emit(g).start()
    place = lax.broadcasted_iota(jnp.int32, (TILES, LANES), 0)
    shares = jnp.zeros((TILES, LANES), jnp.float32)
    for r in range(ROWS):
        lanes = slice(r * LANES, (r + 1) * LANES)
        heat = state[HEAT_ROW : HEAT_ROW + 1, lanes]
        temp_out[r : r + 1, :] = state[TEMP_ROW : TEMP_ROW + 1, lanes]
        rhs_ref[r : r + 1, :] = flow_ref[r : r + 1, :] + heat
        shares += jnp.where(place == owners[0, r // 2], heat * heat, 0.0)
    for o in range(TILES):
        share_ref[o] = shares[o : o + 1, :]
    for g in range(GROUPS):
        emit(g).wait()


def chemistry(chem, temp, flow, counts, owners, weight, molar, factor, energy, release):
    vmem = pl.BlockSpec(memory_space=pltpu.VMEM)
    smem = pl.BlockSpec(memory_space=pltpu.SMEM)
    hbm = pl.BlockSpec(memory_space=pl.ANY)
    f32 = jnp.float32
    return pl.pallas_call(
        chemistry_kernel,
        name="chemistry",
        out_shape=(
            jax.ShapeDtypeStruct((NS, ROWS, LANES), f32),
            jax.ShapeDtypeStruct((ROWS, LANES), f32),
            jax.ShapeDtypeStruct((ROWS, LANES), f32),
            jax.ShapeDtypeStruct((TILES, 1, LANES), f32),
        ),
        in_specs=[smem, smem, hbm, vmem, vmem, vmem, vmem, vmem, vmem, vmem],
        out_specs=(hbm, vmem, vmem, vmem),
        scratch_shapes=[
            pltpu.VMEM((GROUPS, NS, GROUP_ROWS, LANES), f32),
            pltpu.VMEM((GROUPS, NS, GROUP_ROWS, LANES), f32),
            pltpu.VMEM((STATE, ROWS * LANES), f32),
            pltpu.VMEM((STATE, 384), f32),
            pltpu.VMEM((REACT, 256), f32),
            pltpu.VMEM((REACT, 256), jnp.bfloat16),
            pltpu.VMEM((112, 384), jnp.bfloat16),
            pltpu.VMEM((STATE, 384), jnp.bfloat16),
            pltpu.VMEM((1, 384), f32),
            pltpu.SemaphoreType.DMA((GROUPS,)),
            pltpu.SemaphoreType.DMA((GROUPS,)),
        ],
    )(
        counts,
        owners,
        chem,
        temp,
        flow,
        weight.T,
        molar.T,
        factor,
        energy,
        release,
    )


SIDES = tuple((a, b) for a in (-1, 0, 1) for b in (-1, 0, 1) if (a, b) != (0, 0))


def shifted(x, by, axis):
    return pltpu.roll(x, by % x.shape[axis], axis)


def beside(u, d):
    return (shifted(u, d, 0) + shifted(u, -d, 0)) + (shifted(u, d, 1) + shifted(u, -d, 1))


def pooled(x, d, row_first, lane_first):
    x = x + jnp.where(row_first, shifted(x, -d, 0), shifted(x, d, 0))
    return x + jnp.where(lane_first, shifted(x, -d, 1), shifted(x, d, 1))


def projection(rhs, inside):
    rows = lax.broadcasted_iota(jnp.int32, rhs.shape, 0)
    lanes = lax.broadcasted_iota(jnp.int32, rhs.shape, 1)
    weigh = jnp.where(inside, 0.2, 0.0)

    def sweep(u, f, d):
        return 0.2 * u + weigh * (f + beside(u, d))

    f0 = rhs
    u0 = sweep(weigh * f0, f0, 1)
    r0 = f0 - (4.0 * u0 - beside(u0, 1))
    f1 = pooled(r0, 1, (rows & 1) == 0, (lanes & 1) == 0)
    u1 = sweep(weigh * f1, f1, 2)
    r1 = f1 - (4.0 * u1 - beside(u1, 2))
    f2 = pooled(r1, 2, (rows & 2) == 0, (lanes & 2) == 0)
    u2 = weigh * f2
    for _ in range(3):
        u2 = sweep(u2, f2, 4)
    u1 = u1 + u2
    for _ in range(2):
        u1 = sweep(u1, f1, 2)
    u0 = u0 + u1
    for _ in range(2):
        u0 = sweep(u0, f0, 1)
    return u0


def project_kernel(
    gx, gy, rhs_ref, share_ref, field_ref, burden_ref, around, parts, send, recv, part_send, part_recv
):
    i = lax.axis_index("gx")
    j = lax.axis_index("gy")

    def there(a, b):
        here = [i + a >= 0] if a < 0 else [i + a < gx] if a > 0 else []
        here += [j + b >= 0] if b < 0 else [j + b < gy] if b > 0 else []
        return functools.reduce(jnp.logical_and, here)

    def halo(n):
        a, b = SIDES[n]
        return pltpu.make_async_remote_copy(
            src_ref=rhs_ref,
            dst_ref=around.at[len(SIDES) - 1 - n],
            send_sem=send.at[n],
            recv_sem=recv.at[len(SIDES) - 1 - n],
            device_id={"gx": i + a, "gy": j + b},
            device_id_type=MESH,
        )

    def part(d):
        peer = lax.rem(i + d, gx)
        return pltpu.make_async_remote_copy(
            src_ref=share_ref.at[peer],
            dst_ref=parts.at[d],
            send_sem=part_send.at[d],
            recv_sem=part_recv.at[d],
            device_id={"gx": peer, "gy": j},
            device_id_type=MESH,
        )

    barrier = pltpu.get_barrier_semaphore()
    expected = jnp.int32(gx - 1)
    for d in range(1, gx):
        pl.semaphore_signal(
            barrier, inc=1, device_id={"gx": lax.rem(i + d, gx), "gy": j}, device_id_type=MESH
        )
    for a, b in SIDES:
        if b == 0:
            continue
        expected += there(a, b).astype(jnp.int32)

        @pl.when(there(a, b))
        def _(a=a, b=b):
            pl.semaphore_signal(
                barrier, inc=1, device_id={"gx": i + a, "gy": j + b}, device_id_type=MESH
            )

    pl.semaphore_wait(barrier, expected)

    for n, (a, b) in enumerate(SIDES):

        @pl.when(there(a, b))
        def _(n=n):
            halo(n).start()

    for d in range(1, gx):
        part(d).start()

    for n, (a, b) in enumerate(SIDES):
        @pl.when(there(a, b))
        def _(n=n, a=a, b=b):
            pltpu.make_async_remote_copy(
                src_ref=rhs_ref,
                dst_ref=around.at[n],
                send_sem=send.at[n],
                recv_sem=recv.at[n],
                device_id={"gx": i + a, "gy": j + b},
                device_id_type=MESH,
            ).wait_recv()

    blocks = {side: around[n] for n, side in enumerate(SIDES)}
    blocks[(0, 0)] = rhs_ref[...]
    west, middle, east = (
        pltpu.roll(jnp.concatenate([blocks[(a, b)] for a in (-1, 0, 1)], axis=0), 64, 1)
        for b in (-1, 0, 1)
    )
    lane = lax.broadcasted_iota(jnp.int32, west.shape, 1)
    grid = jnp.concatenate(
        [jnp.where(lane < 64, west, middle), jnp.where(lane < 64, middle, east)], axis=1
    )
    rows = lax.broadcasted_iota(jnp.int32, grid.shape, 0) + (i - 1) * ROWS
    lanes = lax.broadcasted_iota(jnp.int32, grid.shape, 1) + (j * LANES - 64)
    inside = (rows >= 0) & (rows < gx * ROWS) & (lanes >= 0) & (lanes < gy * LANES)
    field = projection(jnp.where(inside, grid, 0.0), inside)[ROWS : 2 * ROWS]
    left, right = pltpu.roll(field[:, 0:128], 64, 1), pltpu.roll(field[:, 128:256], 64, 1)
    lane = lax.broadcasted_iota(jnp.int32, left.shape, 1)
    field_ref[...] = jnp.where(lane < 64, left, right)

    total = share_ref[i]
    for d in range(1, gx):
        part(d).wait_recv()
        total = total + parts[d]
    burden_ref[...] = jnp.sum(total, axis=1, keepdims=True) / float(ROWS * LANES)

    for n, (a, b) in enumerate(SIDES):

        @pl.when(there(a, b))
        def _(n=n):
            halo(n).wait_send()

    for d in range(1, gx):
        part(d).wait_send()


def project(rhs, shares, gx, gy):
    vmem = pl.BlockSpec(memory_space=pltpu.VMEM)
    f32 = jnp.float32
    return pl.pallas_call(
        functools.partial(project_kernel, gx, gy),
        name="project",
        out_shape=(
            jax.ShapeDtypeStruct((ROWS, LANES), f32),
            jax.ShapeDtypeStruct((1, 1), f32),
        ),
        in_specs=[vmem, vmem],
        out_specs=(vmem, vmem),
        scratch_shapes=[
            pltpu.VMEM((len(SIDES), ROWS, LANES), f32),
            pltpu.VMEM((16, 1, LANES), f32),
            pltpu.SemaphoreType.DMA((len(SIDES),)),
            pltpu.SemaphoreType.DMA((len(SIDES),)),
            pltpu.SemaphoreType.DMA((16,)),
            pltpu.SemaphoreType.DMA((16,)),
        ],
        compiler_params=pltpu.CompilerParams(collective_id=0, has_side_effects=True),
    )(rhs, shares)


def solution(mesh):
    gx, gy = mesh.shape["gx"], mesh.shape["gy"]

    def shards(chem, temp, flow, counts, owners, weight, molar, factor, energy, release):
        chem_new, temp_new, rhs, shares = chemistry(
            chem, temp, flow, counts, owners, weight, molar, factor, energy, release
        )
        field, burden = project(rhs, shares, gx, gy)
        return chem_new, temp_new, field, burden

    return jax.shard_map(
        shards,
        mesh=mesh,
        in_specs=(
            P(None, "gx", "gy"),
            P("gx", "gy"),
            P("gx", "gy"),
            P("gx", "gy"),
            P("gx", "gy"),
            P(),
            P(),
            P(),
            P(),
            P(),
        ),
        out_specs=(P(None, "gx", "gy"), P("gx", "gy"), P("gx", "gy"), P("gx", "gy")),
        check_vma=False,
    )
```

```python
import functools

import jax
import jax.numpy as jnp
from jax import lax
from jax.experimental import pallas as pl
from jax.experimental.pallas import tpu as pltpu
from jax.sharding import PartitionSpec as P

NS = 53
NR = 325
MAXSUB = 4
TILES = 16
ROWS = 32
LANES = 128
STATE = 64
REACT = 336
TEMP_ROW = 53
HEAT_ROW = 54
GROUPS = 4
STRIP = 32
GROUP_ROWS = ROWS // GROUPS
step_time = 0.4
MESH = pl.DeviceIdType.MESH
KEPT = pltpu.VMEM


def halves(x):
    top = x.astype(jnp.bfloat16)
    rest = (x - top.astype(jnp.float32)).astype(jnp.bfloat16)
    return top, rest


SIDES = tuple((a, b) for a in (-1, 0, 1) for b in (-1, 0, 1) if (a, b) != (0, 0))


def shifted(x, by, axis):
    return pltpu.roll(x, by % x.shape[axis], axis)


def beside(u, d):
    return (shifted(u, d, 0) + shifted(u, -d, 0)) + (shifted(u, d, 1) + shifted(u, -d, 1))


def pooled(x, d, row_first, lane_first):
    x = x + jnp.where(row_first, shifted(x, -d, 0), shifted(x, d, 0))
    return x + jnp.where(lane_first, shifted(x, -d, 1), shifted(x, d, 1))


def projection(rhs, inside):
    rows = lax.broadcasted_iota(jnp.int32, rhs.shape, 0)
    lanes = lax.broadcasted_iota(jnp.int32, rhs.shape, 1)
    weigh = jnp.where(inside, 0.2, 0.0)

    def sweep(u, f, d):
        return 0.2 * u + weigh * (f + beside(u, d))

    f0 = rhs
    u0 = sweep(weigh * f0, f0, 1)
    r0 = f0 - (4.0 * u0 - beside(u0, 1))
    f1 = pooled(r0, 1, (rows & 1) == 0, (lanes & 1) == 0)
    u1 = sweep(weigh * f1, f1, 2)
    r1 = f1 - (4.0 * u1 - beside(u1, 2))
    f2 = pooled(r1, 2, (rows & 2) == 0, (lanes & 2) == 0)
    u2 = weigh * f2
    for _ in range(3):
        u2 = sweep(u2, f2, 4)
    u1 = u1 + u2
    for _ in range(2):
        u1 = sweep(u1, f1, 2)
    u0 = u0 + u1
    for _ in range(2):
        u0 = sweep(u0, f0, 1)
    return u0


def peers(gx, gy):
    i = lax.axis_index("gx")
    j = lax.axis_index("gy")

    def there(a, b):
        here = [i + a >= 0] if a < 0 else [i + a < gx] if a > 0 else []
        here += [j + b >= 0] if b < 0 else [j + b < gy] if b > 0 else []
        return functools.reduce(jnp.logical_and, here)

    return i, j, there


def strip(block, start):
    lane = lax.broadcasted_iota(jnp.int32, (8, LANES), 1)
    packed = jnp.zeros((8, LANES), jnp.float32)
    for k in range(GROUPS):
        moved = pltpu.roll(block[8 * k : 8 * k + 8], (STRIP * k - start) % LANES, 1)
        packed = jnp.where((lane >= STRIP * k) & (lane < STRIP * (k + 1)), moved, packed)
    return packed


def react_kernel(
    gx,
    gy,
    counts,
    owners,
    chem_hbm,
    temp_hbm,
    flow_hbm,
    weight_hbm,
    molar_hbm,
    factor_ref,
    energy_ref,
    release_ref,
    out_buf,
    temp_out,
    rhs_ref,
    rows_in,
    strips_in,
    parts,
    chem_buf,
    temp_ref,
    flow_ref,
    weight_ref,
    molar_ref,
    state,
    wide,
    energy_cols,
    first,
    second,
    pad,
    strips,
    shares,
    in_sem,
    load_sem,
    send,
    recv,
    part_send,
    part_recv,
):
    i, j, there = peers(gx, gy)

    def fetch(g):
        return pltpu.make_async_copy(
            chem_hbm.at[:, pl.ds(g * GROUP_ROWS, GROUP_ROWS), :], chem_buf.at[g], in_sem.at[g]
        )

    loads = [
        pltpu.make_async_copy(source, target, load_sem.at[n])
        for n, (source, target) in enumerate(
            (
                (weight_hbm, weight_ref),
                (molar_hbm, molar_ref),
                (temp_hbm, temp_ref),
                (flow_hbm, flow_ref),
            )
        )
    ]
    for load in loads[:2]:
        load.start()
    for g in range(GROUPS):
        fetch(g).start()
    for load in loads[2:]:
        load.start()

    barrier = pltpu.get_barrier_semaphore()
    expected = jnp.int32(gx - 1)
    for d in range(1, gx):
        pl.semaphore_signal(
            barrier, inc=1, device_id={"gx": lax.rem(i + d, gx), "gy": j}, device_id_type=MESH
        )
    for a, b in SIDES:
        if b == 0:
            continue
        expected += there(a, b).astype(jnp.int32)

        @pl.when(there(a, b))
        def _(a=a, b=b):
            pl.semaphore_signal(
                barrier, inc=1, device_id={"gx": i + a, "gy": j + b}, device_id_type=MESH
            )

    pad[...] = jnp.zeros_like(pad)
    pad[0:1, 0:NR] = energy_ref[...].reshape(1, NR) * -1.4426950408889634
    columns = jnp.broadcast_to(pad[...], (LANES, 384)).T[0:REACT]
    energy_cols[:, 0:128] = columns
    energy_cols[:, 128:256] = columns
    wide[...] = jnp.zeros_like(wide)

    loads[0].wait()
    wide[0:NS, 0:NR] = weight_ref[...] * jnp.exp(factor_ref[...].reshape(1, NR))
    whole = wide[:, 0:384]
    top = whole.astype(jnp.bfloat16).astype(jnp.float32)
    both = jnp.concatenate([top, whole - top], axis=0).T[0:REACT].astype(jnp.bfloat16)
    first[:, 0:128] = both
    first[:, 128:256] = both

    loads[1].wait()
    wide[0:NS, 0:NR] = molar_ref[...]
    wide[TEMP_ROW : TEMP_ROW + 1, 0:NR] = release_ref[...].reshape(1, NR)
    wide[HEAT_ROW : HEAT_ROW + 1, 0:NR] = release_ref[...].reshape(1, NR)
    whole = wide[0:56, :]
    top = whole.astype(jnp.bfloat16).astype(jnp.float32)
    twice = top + pltpu.roll(top, REACT, 1)
    second[...] = jnp.concatenate([twice, whole - top], axis=0).astype(jnp.bfloat16)

    state[NS:STATE, :] = jnp.zeros((STATE - NS, ROWS * LANES), jnp.float32)
    for g in range(GROUPS):
        fetch(g).wait()
        rows = chem_buf.at[g].reshape(NS * GROUP_ROWS, LANES)
        for r in range(GROUP_ROWS):
            lanes = pl.ds((g * GROUP_ROWS + r) * LANES, LANES)
            state[0:NS, lanes] = rows[pl.ds(r, NS, stride=GROUP_ROWS), :]
    loads[2].wait()
    for r in range(ROWS):
        state[TEMP_ROW : TEMP_ROW + 1, r * LANES : (r + 1) * LANES] = temp_ref[r : r + 1, :]

    def turn_body(turn, carry):
        def before(t):
            now = state[:, t * 256 : (t + 1) * 256]
            top, rest = halves(now)
            taken = jnp.concatenate([top, top, rest, rest], axis=0)
            return jnp.dot(first[...], taken, preferred_element_type=jnp.float32)

        def after(t, progress):
            cells = pl.ds(t * 256, 256)
            inverse = 1.0 / (1.0 + jnp.abs(state[TEMP_ROW : TEMP_ROW + 1, cells]))
            flux = jnp.exp2(energy_cols[...] * inverse) * progress
            mixed = jnp.concatenate(halves(flux), axis=0)
            made = jnp.dot(second[:, 0:512], mixed[0:512], preferred_element_type=jnp.float32)
            more = jnp.dot(
                second[0:64, 512:672], mixed[512:672], preferred_element_type=jnp.float32
            )
            change = made[0:56] + made[56:112] + more[0:56]
            count = jnp.full((1, 256), counts[0, t], jnp.int32)
            width = step_time / count.astype(jnp.float32)
            delta = jnp.where(turn < count, width, 0.0)
            state[0:56, cells] += delta * change

        ahead = before(0)
        for t in range(TILES):
            progress = ahead
            if t + 1 < TILES:
                ahead = before(t + 1)
            after(t, progress)
        return carry

    lax.fori_loop(0, MAXSUB, turn_body, 0)

    loads[3].wait()
    place = lax.broadcasted_iota(jnp.int32, (TILES, LANES), 0)
    share = jnp.zeros((TILES, LANES), jnp.float32)
    for r in range(ROWS):
        lanes = slice(r * LANES, (r + 1) * LANES)
        heat = state[HEAT_ROW : HEAT_ROW + 1, lanes]
        rhs_ref[r : r + 1, :] = flow_ref[r : r + 1, :] + heat
        share += jnp.where(place == owners[0, r // 2], heat * heat, 0.0)
    for o in range(TILES):
        shares[o] = share[o : o + 1, :]
    block = rhs_ref[...]
    strips[0] = strip(block, 0)
    strips[1] = strip(block, LANES - STRIP)

    pl.semaphore_wait(barrier, expected)

    def halo(n):
        a, b = SIDES[n]
        slot = len(SIDES) - 1 - n
        return pltpu.make_async_remote_copy(
            src_ref=rhs_ref if b == 0 else strips.at[0 if b < 0 else 1],
            dst_ref=rows_in.at[0 if a > 0 else 1] if b == 0 else strips_in.at[slot],
            send_sem=send.at[n],
            recv_sem=recv.at[slot],
            device_id={"gx": i + a, "gy": j + b},
            device_id_type=MESH,
        )

    def part(d):
        peer = lax.rem(i + d, gx)
        return pltpu.make_async_remote_copy(
            src_ref=shares.at[peer],
            dst_ref=parts.at[d],
            send_sem=part_send.at[d],
            recv_sem=part_recv.at[d],
            device_id={"gx": peer, "gy": j},
            device_id_type=MESH,
        )

    for n in (0, 2, 5, 7, 1, 6, 3, 4):

        @pl.when(there(*SIDES[n]))
        def _(n=n):
            halo(n).start()

    for d in range(1, gx):
        part(d).start()

    parts[0] = shares[i]
    for r in range(ROWS):
        temp_out[r : r + 1, :] = state[TEMP_ROW : TEMP_ROW + 1, r * LANES : (r + 1) * LANES]
    for g in range(GROUPS):
        rows = out_buf.at[g].reshape(NS * GROUP_ROWS, LANES)
        for r in range(GROUP_ROWS):
            lanes = pl.ds((g * GROUP_ROWS + r) * LANES, LANES)
            rows[pl.ds(r, NS, stride=GROUP_ROWS), :] = state[0:NS, lanes]

    for n in range(len(SIDES)):
        @pl.when(there(*SIDES[n]))
        def _(n=n):
            halo(len(SIDES) - 1 - n).wait_recv()

    for d in range(1, gx):
        part(d).wait_recv()

    for n in range(len(SIDES)):

        @pl.when(there(*SIDES[n]))
        def _(n=n):
            halo(n).wait_send()

    for d in range(1, gx):
        part(d).wait_send()


def react(gx, gy, chem, temp, flow, counts, owners, weight, molar, factor, energy, release):
    vmem = pl.BlockSpec(memory_space=pltpu.VMEM)
    smem = pl.BlockSpec(memory_space=pltpu.SMEM)
    hbm = pl.BlockSpec(memory_space=pl.ANY)
    f32 = jnp.float32
    sides = len(SIDES)
    dma = pltpu.SemaphoreType.DMA
    return pl.pallas_call(
        functools.partial(react_kernel, gx, gy),
        name="react",
        out_shape=(
            KEPT((GROUPS, NS, GROUP_ROWS, LANES), f32),
            KEPT((ROWS, LANES), f32),
            KEPT((ROWS, LANES), f32),
            KEPT((2, ROWS, LANES), f32),
            KEPT((sides, 8, LANES), f32),
            KEPT((gx, 1, LANES), f32),
        ),
        in_specs=[smem, smem] + [hbm] * 5 + [vmem] * 3,
        out_specs=(vmem,) * 6,
        scratch_shapes=[
            pltpu.VMEM((GROUPS, NS, GROUP_ROWS, LANES), f32),
            pltpu.VMEM((ROWS, LANES), f32),
            pltpu.VMEM((ROWS, LANES), f32),
            pltpu.VMEM((NS, NR), f32),
            pltpu.VMEM((NS, NR), f32),
            pltpu.VMEM((STATE, ROWS * LANES), f32),
            pltpu.VMEM((STATE, 768), f32),
            pltpu.VMEM((REACT, 256), f32),
            pltpu.VMEM((REACT, 256), jnp.bfloat16),
            pltpu.VMEM((112, 768), jnp.bfloat16),
            pltpu.VMEM((1, 384), f32),
            pltpu.VMEM((2, 8, LANES), f32),
            pltpu.VMEM((TILES, 1, LANES), f32),
            dma((GROUPS,)),
            dma((4,)),
            dma((sides,)),
            dma((sides,)),
            dma((gx,)),
            dma((gx,)),
        ],
        compiler_params=pltpu.CompilerParams(collective_id=0, has_side_effects=True),
    )(counts, owners, chem, temp, flow, weight.T, molar.T, factor, energy, release)


def project_kernel(
    gx,
    gy,
    chem_ref,
    temp_ref,
    rhs_ref,
    rows_in,
    strips_in,
    parts,
    chem_out,
    temp_out,
    field_ref,
    burden_ref,
    sem,
):
    i, j, _ = peers(gx, gy)
    stores = [
        pltpu.make_async_copy(
            chem_ref.at[g], chem_out.at[:, pl.ds(g * GROUP_ROWS, GROUP_ROWS), :], sem.at[g]
        )
        for g in range(GROUPS)
    ]
    stores.append(pltpu.make_async_copy(temp_ref, temp_out, sem.at[GROUPS]))
    for store in stores:
        store.start()

    total = parts[0]
    for d in range(1, gx):
        total = total + parts[d]
    burden_ref[...] = jnp.sum(total, axis=1, keepdims=True) / float(ROWS * LANES)

    middle = jnp.concatenate([rows_in[0], rhs_ref[...], rows_in[1]], axis=0)
    middle = pltpu.roll(middle, 64, 1)

    def beside_column(b, at):
        column = []
        for a in (-1, 0, 1):
            packed = strips_in[SIDES.index((a, b))]
            column += [pltpu.roll(packed, (at - STRIP * k) % LANES, 1) for k in range(GROUPS)]
        return jnp.concatenate(column, axis=0)

    lane = lax.broadcasted_iota(jnp.int32, middle.shape, 1)
    left = jnp.where(lane < 64, beside_column(-1, STRIP), middle)
    right = jnp.where(lane < 64, middle, beside_column(1, 64))
    grid = jnp.concatenate([left, right], axis=1)
    rows = lax.broadcasted_iota(jnp.int32, grid.shape, 0)
    lanes = lax.broadcasted_iota(jnp.int32, grid.shape, 1)
    known = (lanes >= 64 - STRIP) & (lanes < 192 + STRIP)
    rows, lanes = rows + (i - 1) * ROWS, lanes + (j * LANES - 64)
    inside = (rows >= 0) & (rows < gx * ROWS) & (lanes >= 0) & (lanes < gy * LANES) & known
    field = projection(jnp.where(inside, grid, 0.0), inside)[ROWS : 2 * ROWS]
    left, right = pltpu.roll(field[:, 0:128], 64, 1), pltpu.roll(field[:, 128:256], 64, 1)
    lane = lax.broadcasted_iota(jnp.int32, left.shape, 1)
    field_ref[...] = jnp.where(lane < 64, left, right)
    for store in stores:
        store.wait()


def held(x):
    return pltpu.with_memory_space_constraint(x, pltpu.VMEM)


def project(gx, gy, *arrays):
    vmem = pl.BlockSpec(memory_space=pltpu.VMEM)
    hbm = pl.BlockSpec(memory_space=pl.ANY)
    f32 = jnp.float32
    return pl.pallas_call(
        functools.partial(project_kernel, gx, gy),
        name="project",
        out_shape=(
            jax.ShapeDtypeStruct((NS, ROWS, LANES), f32),
            jax.ShapeDtypeStruct((ROWS, LANES), f32),
            jax.ShapeDtypeStruct((ROWS, LANES), f32),
            jax.ShapeDtypeStruct((1, 1), f32),
        ),
        in_specs=[vmem] * len(arrays),
        out_specs=(hbm, hbm, vmem, vmem),
        scratch_shapes=[pltpu.SemaphoreType.DMA((GROUPS + 1,))],
    )(*(held(x) for x in arrays))


def solution(mesh):
    gx, gy = mesh.shape["gx"], mesh.shape["gy"]

    def shards(*args):
        return project(gx, gy, *react(gx, gy, *args))

    return jax.shard_map(
        shards,
        mesh=mesh,
        in_specs=(
            P(None, "gx", "gy"),
            P("gx", "gy"),
            P("gx", "gy"),
            P("gx", "gy"),
            P("gx", "gy"),
            P(),
            P(),
            P(),
            P(),
            P(),
        ),
        out_specs=(P(None, "gx", "gy"), P("gx", "gy"), P("gx", "gy"), P("gx", "gy")),
        check_vma=False,
    )
```

```python
import functools

import jax
import jax.numpy as jnp
from jax import lax
from jax.experimental import pallas as pl
from jax.experimental.pallas import tpu as pltpu
from jax.sharding import PartitionSpec as P

NS = 53
NR = 325
MAXSUB = 4
TILES = 16
ROWS = 32
LANES = 128
STATE = 64
REACT = 336
AHEAD = 2
BEHIND = 0
UNROLL = 1
TEMP_ROW = 53
HEAT_ROW = 54
GROUPS = 4
STRIP = 32
GROUP_ROWS = ROWS // GROUPS
step_time = 0.4
MESH = pl.DeviceIdType.MESH
KEPT = pltpu.VMEM


def halves(x):
    top = x.astype(jnp.bfloat16)
    rest = (x - top.astype(jnp.float32)).astype(jnp.bfloat16)
    return top, rest


SIDES = tuple((a, b) for a in (-1, 0, 1) for b in (-1, 0, 1) if (a, b) != (0, 0))


def shifted(x, by, axis):
    return pltpu.roll(x, by % x.shape[axis], axis)


def beside(u, d):
    return (shifted(u, d, 0) + shifted(u, -d, 0)) + (shifted(u, d, 1) + shifted(u, -d, 1))


def pooled(x, d, row_first, lane_first):
    x = x + jnp.where(row_first, shifted(x, -d, 0), shifted(x, d, 0))
    return x + jnp.where(lane_first, shifted(x, -d, 1), shifted(x, d, 1))


def projection(rhs, inside):
    rows = lax.broadcasted_iota(jnp.int32, rhs.shape, 0)
    lanes = lax.broadcasted_iota(jnp.int32, rhs.shape, 1)
    weigh = jnp.where(inside, 0.2, 0.0)

    def sweep(u, f, d, w):
        return 0.2 * u + w * (f + beside(u, d))

    f0 = rhs
    u0 = sweep(weigh * f0, f0, 1, weigh)
    r0 = f0 - (4.0 * u0 - beside(u0, 1))
    f1 = pooled(r0, 1, (rows & 1) == 0, (lanes & 1) == 0)
    u1 = sweep(weigh * f1, f1, 2, weigh)
    r1 = f1 - (4.0 * u1 - beside(u1, 2))
    f2 = pooled(r1, 2, (rows & 2) == 0, (lanes & 2) == 0)
    u2 = sweep(weigh * f2, f2, 4, weigh)
    u2, f2, w = u2[8:88], f2[8:88], weigh[8:88]
    u2 = sweep(u2, f2, 4, w)
    u2, f2, w = u2[8:72], f2[8:72], weigh[16:80]
    u2 = sweep(u2, f2, 4, w)[8:56]
    middle = slice(24, 72)
    f0, f1, w = f0[middle], f1[middle], weigh[middle]
    u1 = u1[middle] + u2
    for _ in range(2):
        u1 = sweep(u1, f1, 2, w)
    u0 = u0[middle] + u1
    for _ in range(2):
        u0 = sweep(u0, f0, 1, w)
    return u0[8:40]


def peers(gx, gy):
    i = lax.axis_index("gx")
    j = lax.axis_index("gy")

    def there(a, b):
        here = [i + a >= 0] if a < 0 else [i + a < gx] if a > 0 else []
        here += [j + b >= 0] if b < 0 else [j + b < gy] if b > 0 else []
        return functools.reduce(jnp.logical_and, here)

    return i, j, there


def strip(block, start):
    lane = lax.broadcasted_iota(jnp.int32, (8, LANES), 1)
    packed = jnp.zeros((8, LANES), jnp.float32)
    for k in range(GROUPS):
        moved = pltpu.roll(block[8 * k : 8 * k + 8], (STRIP * k - start) % LANES, 1)
        packed = jnp.where((lane >= STRIP * k) & (lane < STRIP * (k + 1)), moved, packed)
    return packed


def react_kernel(
    gx,
    gy,
    counts,
    owners,
    chem_hbm,
    temp_hbm,
    flow_hbm,
    weight_hbm,
    molar_hbm,
    factor_hbm,
    energy_hbm,
    release_hbm,
    out_buf,
    temp_out,
    rhs_ref,
    rows_in,
    strips_in,
    parts,
    chem_buf,
    temp_ref,
    flow_ref,
    weight_ref,
    molar_ref,
    factor_ref,
    energy_ref,
    release_ref,
    state,
    wide,
    energy_cols,
    first,
    second,
    pad,
    strips,
    shares,
    in_sem,
    load_sem,
    send,
    recv,
    part_send,
    part_recv,
):
    i, j, there = peers(gx, gy)

    def fetch(g):
        return pltpu.make_async_copy(
            chem_hbm.at[:, pl.ds(g * GROUP_ROWS, GROUP_ROWS), :], chem_buf.at[g], in_sem.at[g]
        )

    loads = [
        pltpu.make_async_copy(source, target, load_sem.at[n])
        for n, (source, target) in enumerate(
            (
                (energy_hbm, energy_ref),
                (factor_hbm, factor_ref),
                (weight_hbm, weight_ref),
                (release_hbm, release_ref),
                (molar_hbm, molar_ref),
                (temp_hbm, temp_ref),
                (flow_hbm, flow_ref),
            )
        )
    ]
    for load in loads[:5]:
        load.start()
    for g in range(GROUPS):
        fetch(g).start()
    for load in loads[5:]:
        load.start()

    pad[...] = jnp.zeros_like(pad)
    wide[...] = jnp.zeros_like(wide)
    state[NS:STATE, :] = jnp.zeros((STATE - NS, ROWS * LANES), jnp.float32)

    barrier = pltpu.get_barrier_semaphore()
    expected = jnp.int32(gx - 1)
    for d in range(1, gx):
        pl.semaphore_signal(
            barrier, inc=1, device_id={"gx": lax.rem(i + d, gx), "gy": j}, device_id_type=MESH
        )
    for a, b in SIDES:
        if b == 0:
            continue
        expected += there(a, b).astype(jnp.int32)

        @pl.when(there(a, b))
        def _(a=a, b=b):
            pl.semaphore_signal(
                barrier, inc=1, device_id={"gx": i + a, "gy": j + b}, device_id_type=MESH
            )

    loads[0].wait()
    pad[0:1, 0:NR] = energy_ref[...].reshape(1, NR) * -1.4426950408889634
    columns = jnp.broadcast_to(pad[...], (LANES, 384)).T[0:REACT]
    energy_cols[:, 0:128] = columns
    energy_cols[:, 128:256] = columns

    loads[1].wait()
    loads[2].wait()
    wide[0:NS, 0:NR] = weight_ref[...] * jnp.exp(factor_ref[...].reshape(1, NR))
    whole = wide[:, 0:384]
    top = whole.astype(jnp.bfloat16).astype(jnp.float32)
    both = jnp.concatenate([top, whole - top], axis=0).T[0:REACT].astype(jnp.bfloat16)
    first[:, 0:128] = both
    first[:, 128:256] = both

    loads[3].wait()
    loads[4].wait()
    wide[0:NS, 0:NR] = molar_ref[...]
    wide[TEMP_ROW : TEMP_ROW + 1, 0:NR] = release_ref[...].reshape(1, NR)
    wide[HEAT_ROW : HEAT_ROW + 1, 0:NR] = release_ref[...].reshape(1, NR)
    whole = wide[0:56, :]
    top = whole.astype(jnp.bfloat16).astype(jnp.float32)
    twice = top + pltpu.roll(top, REACT, 1)
    second[...] = jnp.concatenate([twice, whole - top], axis=0).astype(jnp.bfloat16)

    for g in range(GROUPS):
        fetch(g).wait()
        rows = chem_buf.at[g].reshape(NS * GROUP_ROWS, LANES)
        for r in range(GROUP_ROWS):
            lanes = pl.ds((g * GROUP_ROWS + r) * LANES, LANES)
            state[0:NS, lanes] = rows[pl.ds(r, NS, stride=GROUP_ROWS), :]
    loads[5].wait()
    for r in range(ROWS):
        state[TEMP_ROW : TEMP_ROW + 1, r * LANES : (r + 1) * LANES] = temp_ref[r : r + 1, :]

    def before(step):
        t = step % TILES
        now = state[:, t * 256 : (t + 1) * 256]
        top, rest = halves(now)
        taken = jnp.concatenate([top, top, rest, rest], axis=0)
        return jnp.dot(first[...], taken, preferred_element_type=jnp.float32)

    def middle(step, progress):
        t = step % TILES
        inverse = 1.0 / (1.0 + jnp.abs(state[TEMP_ROW : TEMP_ROW + 1, t * 256 : (t + 1) * 256]))
        flux = jnp.exp2(energy_cols[...] * inverse) * progress
        mixed = jnp.concatenate(halves(flux), axis=0)
        made = jnp.dot(second[:, 0:512], mixed[0:512], preferred_element_type=jnp.float32)
        more = jnp.dot(second[0:64, 512:672], mixed[512:672], preferred_element_type=jnp.float32)
        return made[0:56] + made[56:112] + more[0:56]

    def finish(turn, step, change):
        t = step % TILES
        count = jnp.full((1, 256), counts[0, t], jnp.int32)
        width = step_time / count.astype(jnp.float32)
        delta = jnp.where(turn + step // TILES < count, width, 0.0)
        state[0:56, t * 256 : (t + 1) * 256] += delta * change

    def turn_body(index, carry):
        ahead, made = {}, {}
        for step in range(-AHEAD, UNROLL * TILES + BEHIND):
            if step + AHEAD < UNROLL * TILES:
                ahead[step + AHEAD] = before(step + AHEAD)
            if 0 <= step < UNROLL * TILES:
                made[step] = middle(step, ahead.pop(step))
            if step >= BEHIND:
                finish(index * UNROLL, step - BEHIND, made.pop(step - BEHIND))
        return carry

    lax.fori_loop(0, MAXSUB // UNROLL, turn_body, 0)

    loads[6].wait()
    place = lax.broadcasted_iota(jnp.int32, (TILES, LANES), 0)
    share = jnp.zeros((TILES, LANES), jnp.float32)
    for r in range(ROWS):
        lanes = slice(r * LANES, (r + 1) * LANES)
        heat = state[HEAT_ROW : HEAT_ROW + 1, lanes]
        rhs_ref[r : r + 1, :] = flow_ref[r : r + 1, :] + heat
        share += jnp.where(place == owners[0, r // 2], heat * heat, 0.0)
    for o in range(TILES):
        shares[o] = share[o : o + 1, :]
    block = rhs_ref[...]
    strips[0] = strip(block, 0)
    strips[1] = strip(block, LANES - STRIP)

    pl.semaphore_wait(barrier, expected)

    def halo(n):
        a, b = SIDES[n]
        slot = len(SIDES) - 1 - n
        return pltpu.make_async_remote_copy(
            src_ref=rhs_ref if b == 0 else strips.at[0 if b < 0 else 1],
            dst_ref=rows_in.at[0 if a > 0 else 1] if b == 0 else strips_in.at[slot],
            send_sem=send.at[n],
            recv_sem=recv.at[slot],
            device_id={"gx": i + a, "gy": j + b},
            device_id_type=MESH,
        )

    def part(d):
        peer = lax.rem(i + d, gx)
        return pltpu.make_async_remote_copy(
            src_ref=shares.at[peer],
            dst_ref=parts.at[d],
            send_sem=part_send,
            recv_sem=part_recv,
            device_id={"gx": peer, "gy": j},
            device_id_type=MESH,
        )

    for d in range(1, gx):
        part(d).start()

    for n in (0, 2, 5, 7, 1, 6, 3, 4):

        @pl.when(there(*SIDES[n]))
        def _(n=n):
            halo(n).start()

    parts[0] = shares[i]
    for r in range(ROWS):
        temp_out[r : r + 1, :] = state[TEMP_ROW : TEMP_ROW + 1, r * LANES : (r + 1) * LANES]
    for g in range(GROUPS):
        rows = out_buf.at[g].reshape(NS * GROUP_ROWS, LANES)
        for r in range(GROUP_ROWS):
            lanes = pl.ds((g * GROUP_ROWS + r) * LANES, LANES)
            rows[pl.ds(r, NS, stride=GROUP_ROWS), :] = state[0:NS, lanes]

    for n in range(len(SIDES)):
        @pl.when(there(*SIDES[n]))
        def _(n=n):
            halo(len(SIDES) - 1 - n).wait_recv()

    pltpu.make_async_copy(parts.at[pl.ds(1, gx - 1)], parts.at[pl.ds(1, gx - 1)], part_recv).wait()

    for n in range(len(SIDES)):

        @pl.when(there(*SIDES[n]))
        def _(n=n):
            halo(n).wait_send()

    pltpu.make_async_copy(shares.at[pl.ds(1, gx - 1)], shares.at[pl.ds(1, gx - 1)], part_send).wait()


def react(gx, gy, chem, temp, flow, counts, owners, weight, molar, factor, energy, release):
    vmem = pl.BlockSpec(memory_space=pltpu.VMEM)
    smem = pl.BlockSpec(memory_space=pltpu.SMEM)
    hbm = pl.BlockSpec(memory_space=pl.ANY)
    f32 = jnp.float32
    sides = len(SIDES)
    dma = pltpu.SemaphoreType.DMA
    return pl.pallas_call(
        functools.partial(react_kernel, gx, gy),
        name="react",
        out_shape=(
            KEPT((GROUPS, NS, GROUP_ROWS, LANES), f32),
            KEPT((ROWS, LANES), f32),
            KEPT((ROWS, LANES), f32),
            KEPT((2, ROWS, LANES), f32),
            KEPT((sides, 8, LANES), f32),
            KEPT((gx, 1, LANES), f32),
        ),
        in_specs=[smem, smem] + [hbm] * 8,
        out_specs=(vmem,) * 6,
        scratch_shapes=[
            pltpu.VMEM((GROUPS, NS, GROUP_ROWS, LANES), f32),
            pltpu.VMEM((ROWS, LANES), f32),
            pltpu.VMEM((ROWS, LANES), f32),
            pltpu.VMEM((NS, NR), f32),
            pltpu.VMEM((NS, NR), f32),
            pltpu.VMEM((NR,), f32),
            pltpu.VMEM((NR,), f32),
            pltpu.VMEM((NR,), f32),
            pltpu.VMEM((STATE, ROWS * LANES), f32),
            pltpu.VMEM((STATE, 768), f32),
            pltpu.VMEM((REACT, 256), f32),
            pltpu.VMEM((REACT, 256), jnp.bfloat16),
            pltpu.VMEM((112, 768), jnp.bfloat16),
            pltpu.VMEM((1, 384), f32),
            pltpu.VMEM((2, 8, LANES), f32),
            pltpu.VMEM((TILES, 1, LANES), f32),
            dma((GROUPS,)),
            dma((7,)),
            dma((sides,)),
            dma((sides,)),
            dma(()),
            dma(()),
        ],
        compiler_params=pltpu.CompilerParams(collective_id=0, has_side_effects=True),
    )(counts, owners, chem, temp, flow, weight.T, molar.T, factor, energy, release)


def project_kernel(
    gx,
    gy,
    chem_ref,
    temp_ref,
    rhs_ref,
    rows_in,
    strips_in,
    parts,
    chem_out,
    temp_out,
    field_ref,
    burden_ref,
    sem,
):
    i, j, _ = peers(gx, gy)
    stores = [
        pltpu.make_async_copy(
            chem_ref.at[g], chem_out.at[:, pl.ds(g * GROUP_ROWS, GROUP_ROWS), :], sem.at[g]
        )
        for g in range(GROUPS)
    ]
    stores.append(pltpu.make_async_copy(temp_ref, temp_out, sem.at[GROUPS]))
    for store in stores:
        store.start()

    total = parts[0]
    for d in range(1, gx):
        total = total + parts[d]
    burden_ref[...] = jnp.sum(total, axis=1, keepdims=True) / float(ROWS * LANES)

    middle = jnp.concatenate([rows_in[0], rhs_ref[...], rows_in[1]], axis=0)
    middle = pltpu.roll(middle, 64, 1)

    def beside_column(b, at):
        column = []
        for a in (-1, 0, 1):
            packed = strips_in[SIDES.index((a, b))]
            column += [pltpu.roll(packed, (at - STRIP * k) % LANES, 1) for k in range(GROUPS)]
        return jnp.concatenate(column, axis=0)

    lane = lax.broadcasted_iota(jnp.int32, middle.shape, 1)
    left = jnp.where(lane < 64, beside_column(-1, STRIP), middle)
    right = jnp.where(lane < 64, middle, beside_column(1, 64))
    grid = jnp.concatenate([left, right], axis=1)
    rows = lax.broadcasted_iota(jnp.int32, grid.shape, 0)
    lanes = lax.broadcasted_iota(jnp.int32, grid.shape, 1)
    known = (lanes >= 64 - STRIP) & (lanes < 192 + STRIP)
    rows, lanes = rows + (i - 1) * ROWS, lanes + (j * LANES - 64)
    inside = (rows >= 0) & (rows < gx * ROWS) & (lanes >= 0) & (lanes < gy * LANES) & known
    field = projection(jnp.where(inside, grid, 0.0), inside)
    left, right = pltpu.roll(field[:, 0:128], 64, 1), pltpu.roll(field[:, 128:256], 64, 1)
    lane = lax.broadcasted_iota(jnp.int32, left.shape, 1)
    field_ref[...] = jnp.where(lane < 64, left, right)
    for store in stores:
        store.wait()


def held(x):
    return pltpu.with_memory_space_constraint(x, pltpu.VMEM)


def project(gx, gy, *arrays):
    vmem = pl.BlockSpec(memory_space=pltpu.VMEM)
    hbm = pl.BlockSpec(memory_space=pl.ANY)
    f32 = jnp.float32
    return pl.pallas_call(
        functools.partial(project_kernel, gx, gy),
        name="project",
        out_shape=(
            jax.ShapeDtypeStruct((NS, ROWS, LANES), f32),
            jax.ShapeDtypeStruct((ROWS, LANES), f32),
            jax.ShapeDtypeStruct((ROWS, LANES), f32),
            jax.ShapeDtypeStruct((1, 1), f32),
        ),
        in_specs=[vmem] * len(arrays),
        out_specs=(hbm, hbm, vmem, vmem),
        scratch_shapes=[pltpu.SemaphoreType.DMA((GROUPS + 1,))],
    )(*(held(x) for x in arrays))


def solution(mesh):
    gx, gy = mesh.shape["gx"], mesh.shape["gy"]

    def shards(*args):
        return project(gx, gy, *react(gx, gy, *args))

    return jax.shard_map(
        shards,
        mesh=mesh,
        in_specs=(
            P(None, "gx", "gy"),
            P("gx", "gy"),
            P("gx", "gy"),
            P("gx", "gy"),
            P("gx", "gy"),
            P(),
            P(),
            P(),
            P(),
            P(),
        ),
        out_specs=(P(None, "gx", "gy"), P("gx", "gy"), P("gx", "gy"), P("gx", "gy")),
        check_vma=False,
    )
```

```python
import functools

import jax
import jax.numpy as jnp
from jax import lax
from jax.experimental import pallas as pl
from jax.experimental.pallas import tpu as pltpu
from jax.sharding import PartitionSpec as P

NS = 53
NR = 325
MAXSUB = 4
TILES = 16
ROWS = 32
LANES = 128
STATE = 64
REACT = 336
AHEAD = 2
TEMP_ROW = 53
HEAT_ROW = 54
GROUPS = 4
STRIP = 32
GROUP_ROWS = ROWS // GROUPS
step_time = 0.4
MESH = pl.DeviceIdType.MESH
KEPT = pltpu.VMEM


def halves(x):
    top = x.astype(jnp.bfloat16)
    rest = (x - top.astype(jnp.float32)).astype(jnp.bfloat16)
    return top, rest


SIDES = tuple((a, b) for a in (-1, 0, 1) for b in (-1, 0, 1) if (a, b) != (0, 0))


def shifted(x, by, axis):
    return pltpu.roll(x, by % x.shape[axis], axis)


def beside(u, d):
    return (shifted(u, d, 0) + shifted(u, -d, 0)) + (shifted(u, d, 1) + shifted(u, -d, 1))


def pooled(x, d, row_first, lane_first):
    x = x + jnp.where(row_first, shifted(x, -d, 0), shifted(x, d, 0))
    return x + jnp.where(lane_first, shifted(x, -d, 1), shifted(x, d, 1))


def projection(rhs, inside):
    rows = lax.broadcasted_iota(jnp.int32, rhs.shape, 0)
    lanes = lax.broadcasted_iota(jnp.int32, rhs.shape, 1)
    weigh = jnp.where(inside, 0.2, 0.0)

    def sweep(u, f, d, w):
        return 0.2 * u + w * (f + beside(u, d))

    f0 = rhs
    u0 = sweep(weigh * f0, f0, 1, weigh)
    r0 = f0 - (4.0 * u0 - beside(u0, 1))
    f1 = pooled(r0, 1, (rows & 1) == 0, (lanes & 1) == 0)
    u1 = sweep(weigh * f1, f1, 2, weigh)
    r1 = f1 - (4.0 * u1 - beside(u1, 2))
    f2 = pooled(r1, 2, (rows & 2) == 0, (lanes & 2) == 0)
    u2 = sweep(weigh * f2, f2, 4, weigh)
    u2, f2, w = u2[8:88], f2[8:88], weigh[8:88]
    u2 = sweep(u2, f2, 4, w)
    u2, f2, w = u2[8:72], f2[8:72], weigh[16:80]
    u2 = sweep(u2, f2, 4, w)[8:56]
    middle = slice(24, 72)
    f0, f1, w = f0[middle], f1[middle], weigh[middle]
    u1 = u1[middle] + u2
    for _ in range(2):
        u1 = sweep(u1, f1, 2, w)
    u0 = u0[middle] + u1
    for _ in range(2):
        u0 = sweep(u0, f0, 1, w)
    return u0[8:40]


def peers(gx, gy):
    i = lax.axis_index("gx")
    j = lax.axis_index("gy")

    def there(a, b):
        here = [i + a >= 0] if a < 0 else [i + a < gx] if a > 0 else []
        here += [j + b >= 0] if b < 0 else [j + b < gy] if b > 0 else []
        return functools.reduce(jnp.logical_and, here)

    return i, j, there


def strip(block, start):
    lane = lax.broadcasted_iota(jnp.int32, (8, LANES), 1)
    packed = jnp.zeros((8, LANES), jnp.float32)
    for k in range(GROUPS):
        moved = pltpu.roll(block[8 * k : 8 * k + 8], (STRIP * k - start) % LANES, 1)
        packed = jnp.where((lane >= STRIP * k) & (lane < STRIP * (k + 1)), moved, packed)
    return packed


def react_kernel(
    gx,
    gy,
    counts,
    owners,
    chem_hbm,
    temp_hbm,
    flow_hbm,
    weight_hbm,
    molar_hbm,
    factor_hbm,
    energy_hbm,
    release_hbm,
    out_buf,
    temp_out,
    rhs_ref,
    rows_in,
    strips_in,
    parts,
    chem_buf,
    temp_ref,
    flow_ref,
    weight_ref,
    molar_ref,
    factor_ref,
    energy_ref,
    release_ref,
    state,
    wide,
    energy_cols,
    first,
    second,
    pad,
    widths,
    strips,
    shares,
    in_sem,
    load_sem,
    send,
    recv,
    part_send,
    part_recv,
):
    i, j, there = peers(gx, gy)

    def fetch(g):
        return pltpu.make_async_copy(
            chem_hbm.at[:, pl.ds(g * GROUP_ROWS, GROUP_ROWS), :], chem_buf.at[g], in_sem.at[g]
        )

    loads = [
        pltpu.make_async_copy(source, target, load_sem.at[n])
        for n, (source, target) in enumerate(
            (
                (energy_hbm, energy_ref),
                (factor_hbm, factor_ref),
                (weight_hbm, weight_ref),
                (release_hbm, release_ref),
                (molar_hbm, molar_ref),
                (temp_hbm, temp_ref),
                (flow_hbm, flow_ref),
            )
        )
    ]
    for load in loads[:5]:
        load.start()
    for g in range(GROUPS):
        fetch(g).start()
    for load in loads[5:]:
        load.start()

    pad[...] = jnp.zeros_like(pad)
    wide[...] = jnp.zeros_like(wide)
    state[NS:STATE, :] = jnp.zeros((STATE - NS, ROWS * LANES), jnp.float32)

    turns = lax.broadcasted_iota(jnp.int32, (8, 256), 0)
    for t in range(TILES):
        count = jnp.full((8, 256), counts[0, t], jnp.int32)
        width = step_time / count.astype(jnp.float32)
        widths[:, t * 256 : (t + 1) * 256] = jnp.where(turns < count, width, 0.0)

    barrier = pltpu.get_barrier_semaphore()
    expected = jnp.int32(gx - 1)
    for d in range(1, gx):
        pl.semaphore_signal(
            barrier, inc=1, device_id={"gx": lax.rem(i + d, gx), "gy": j}, device_id_type=MESH
        )
    for a, b in SIDES:
        if b == 0:
            continue
        expected += there(a, b).astype(jnp.int32)

        @pl.when(there(a, b))
        def _(a=a, b=b):
            pl.semaphore_signal(
                barrier, inc=1, device_id={"gx": i + a, "gy": j + b}, device_id_type=MESH
            )

    loads[0].wait()
    pad[0:1, 0:NR] = energy_ref[...].reshape(1, NR) * -1.4426950408889634
    columns = jnp.broadcast_to(pad[...], (LANES, 384)).T[0:REACT]
    energy_cols[:, 0:128] = columns
    energy_cols[:, 128:256] = columns

    loads[1].wait()
    loads[2].wait()
    wide[0:NS, 0:NR] = weight_ref[...] * jnp.exp(factor_ref[...].reshape(1, NR))
    whole = wide[:, 0:384]
    top = whole.astype(jnp.bfloat16).astype(jnp.float32)
    both = jnp.concatenate([top, whole - top], axis=0).T[0:REACT].astype(jnp.bfloat16)
    first[:, 0:128] = both
    first[:, 128:256] = both

    loads[3].wait()
    loads[4].wait()
    wide[0:NS, 0:NR] = molar_ref[...]
    wide[TEMP_ROW : TEMP_ROW + 1, 0:NR] = release_ref[...].reshape(1, NR)
    wide[HEAT_ROW : HEAT_ROW + 1, 0:NR] = release_ref[...].reshape(1, NR)
    whole = wide[0:56, :]
    top = whole.astype(jnp.bfloat16).astype(jnp.float32)
    twice = top + pltpu.roll(top, REACT, 1)
    second[...] = jnp.concatenate([twice, whole - top], axis=0).astype(jnp.bfloat16)

    def take(g):
        fetch(g).wait()
        rows = chem_buf.at[g].reshape(NS * GROUP_ROWS, LANES)
        for r in range(GROUP_ROWS):
            lanes = pl.ds((g * GROUP_ROWS + r) * LANES, LANES)
            state[0:NS, lanes] = rows[pl.ds(r, NS, stride=GROUP_ROWS), :]
            row = g * GROUP_ROWS + r
            state[TEMP_ROW : TEMP_ROW + 1, lanes] = temp_ref[row : row + 1, :]

    def before(step):
        t = step % TILES
        now = state[:, t * 256 : (t + 1) * 256]
        top, rest = halves(now)
        taken = jnp.concatenate([top, top, rest, rest], axis=0)
        return jnp.dot(first[...], taken, preferred_element_type=jnp.float32)

    def middle(step, progress):
        t = step % TILES
        inverse = 1.0 / (1.0 + jnp.abs(state[TEMP_ROW : TEMP_ROW + 1, t * 256 : (t + 1) * 256]))
        flux = jnp.exp2(energy_cols[...] * inverse) * progress
        mixed = jnp.concatenate(halves(flux), axis=0)
        made = jnp.dot(second[:, 0:512], mixed[0:512], preferred_element_type=jnp.float32)
        more = jnp.dot(second[0:64, 512:672], mixed[512:672], preferred_element_type=jnp.float32)
        return made[0:56] + made[56:112] + more[0:56]

    def finish(step, change):
        turn, t = divmod(step, TILES)
        cells = slice(t * 256, (t + 1) * 256)
        state[0:56, cells] += widths[turn : turn + 1, cells] * change

    place = lax.broadcasted_iota(jnp.int32, (TILES, LANES), 0)
    share = jnp.zeros((TILES, LANES), jnp.float32)
    steps = MAXSUB * TILES
    ahead = {}
    loads[5].wait()
    loads[6].wait()
    for step in range(-AHEAD, steps):
        if step + AHEAD < steps:
            group, rest = divmod(step + AHEAD, TILES // GROUPS)
            if group < GROUPS and rest == 0:
                take(group)
            ahead[step + AHEAD] = before(step + AHEAD)
        if step >= 0:
            finish(step, middle(step, ahead.pop(step)))
        if step >= steps - TILES:
            t = step % TILES
            for r in (2 * t, 2 * t + 1):
                heat = state[HEAT_ROW : HEAT_ROW + 1, r * LANES : (r + 1) * LANES]
                rhs_ref[r : r + 1, :] = flow_ref[r : r + 1, :] + heat
                share += jnp.where(place == owners[0, t], heat * heat, 0.0)
    for o in range(TILES):
        shares[o] = share[o : o + 1, :]
    block = rhs_ref[...]
    strips[0] = strip(block, 0)
    strips[1] = strip(block, LANES - STRIP)

    pl.semaphore_wait(barrier, expected)

    def halo(n):
        a, b = SIDES[n]
        slot = len(SIDES) - 1 - n
        return pltpu.make_async_remote_copy(
            src_ref=rhs_ref if b == 0 else strips.at[0 if b < 0 else 1],
            dst_ref=rows_in.at[0 if a > 0 else 1] if b == 0 else strips_in.at[slot],
            send_sem=send.at[n],
            recv_sem=recv.at[slot],
            device_id={"gx": i + a, "gy": j + b},
            device_id_type=MESH,
        )

    def part(d):
        peer = lax.rem(i + d, gx)
        return pltpu.make_async_remote_copy(
            src_ref=shares.at[peer],
            dst_ref=parts.at[d],
            send_sem=part_send,
            recv_sem=part_recv,
            device_id={"gx": peer, "gy": j},
            device_id_type=MESH,
        )

    for d in range(1, gx):
        part(d).start()

    for n in (0, 2, 5, 7, 1, 6, 3, 4):

        @pl.when(there(*SIDES[n]))
        def _(n=n):
            halo(n).start()

    parts[0] = shares[i]
    for r in range(ROWS):
        temp_out[r : r + 1, :] = state[TEMP_ROW : TEMP_ROW + 1, r * LANES : (r + 1) * LANES]
    for g in range(GROUPS):
        rows = out_buf.at[g].reshape(NS * GROUP_ROWS, LANES)
        for r in range(GROUP_ROWS):
            lanes = pl.ds((g * GROUP_ROWS + r) * LANES, LANES)
            rows[pl.ds(r, NS, stride=GROUP_ROWS), :] = state[0:NS, lanes]

    for n in range(len(SIDES)):
        @pl.when(there(*SIDES[n]))
        def _(n=n):
            halo(len(SIDES) - 1 - n).wait_recv()

    pltpu.make_async_copy(parts.at[pl.ds(1, gx - 1)], parts.at[pl.ds(1, gx - 1)], part_recv).wait()

    for n in range(len(SIDES)):

        @pl.when(there(*SIDES[n]))
        def _(n=n):
            halo(n).wait_send()

    pltpu.make_async_copy(shares.at[pl.ds(1, gx - 1)], shares.at[pl.ds(1, gx - 1)], part_send).wait()


def react(gx, gy, chem, temp, flow, counts, owners, weight, molar, factor, energy, release):
    vmem = pl.BlockSpec(memory_space=pltpu.VMEM)
    smem = pl.BlockSpec(memory_space=pltpu.SMEM)
    hbm = pl.BlockSpec(memory_space=pl.ANY)
    f32 = jnp.float32
    sides = len(SIDES)
    dma = pltpu.SemaphoreType.DMA
    return pl.pallas_call(
        functools.partial(react_kernel, gx, gy),
        name="react",
        out_shape=(
            KEPT((GROUPS, NS, GROUP_ROWS, LANES), f32),
            KEPT((ROWS, LANES), f32),
            KEPT((ROWS, LANES), f32),
            KEPT((2, ROWS, LANES), f32),
            KEPT((sides, 8, LANES), f32),
            KEPT((gx, 1, LANES), f32),
        ),
        in_specs=[smem, smem] + [hbm] * 8,
        out_specs=(vmem,) * 6,
        scratch_shapes=[
            pltpu.VMEM((GROUPS, NS, GROUP_ROWS, LANES), f32),
            pltpu.VMEM((ROWS, LANES), f32),
            pltpu.VMEM((ROWS, LANES), f32),
            pltpu.VMEM((NS, NR), f32),
            pltpu.VMEM((NS, NR), f32),
            pltpu.VMEM((NR,), f32),
            pltpu.VMEM((NR,), f32),
            pltpu.VMEM((NR,), f32),
            pltpu.VMEM((STATE, ROWS * LANES), f32),
            pltpu.VMEM((STATE, 768), f32),
            pltpu.VMEM((REACT, 256), f32),
            pltpu.VMEM((REACT, 256), jnp.bfloat16),
            pltpu.VMEM((112, 768), jnp.bfloat16),
            pltpu.VMEM((1, 384), f32),
            pltpu.VMEM((8, ROWS * LANES), f32),
            pltpu.VMEM((2, 8, LANES), f32),
            pltpu.VMEM((TILES, 1, LANES), f32),
            dma((GROUPS,)),
            dma((7,)),
            dma((sides,)),
            dma((sides,)),
            dma(()),
            dma(()),
        ],
        compiler_params=pltpu.CompilerParams(collective_id=0, has_side_effects=True),
    )(counts, owners, chem, temp, flow, weight.T, molar.T, factor, energy, release)


def project_kernel(
    gx,
    gy,
    chem_ref,
    temp_ref,
    rhs_ref,
    rows_in,
    strips_in,
    parts,
    chem_out,
    temp_out,
    field_ref,
    burden_ref,
    sem,
):
    i, j, _ = peers(gx, gy)
    stores = [
        pltpu.make_async_copy(
            chem_ref.at[g], chem_out.at[:, pl.ds(g * GROUP_ROWS, GROUP_ROWS), :], sem.at[g]
        )
        for g in range(GROUPS)
    ]
    stores.append(pltpu.make_async_copy(temp_ref, temp_out, sem.at[GROUPS]))
    for store in stores:
        store.start()

    total = parts[0]
    for d in range(1, gx):
        total = total + parts[d]
    burden_ref[...] = jnp.sum(total, axis=1, keepdims=True) / float(ROWS * LANES)

    middle = jnp.concatenate([rows_in[0], rhs_ref[...], rows_in[1]], axis=0)
    middle = pltpu.roll(middle, 64, 1)

    def beside_column(b, at):
        column = []
        for a in (-1, 0, 1):
            packed = strips_in[SIDES.index((a, b))]
            column += [pltpu.roll(packed, (at - STRIP * k) % LANES, 1) for k in range(GROUPS)]
        return jnp.concatenate(column, axis=0)

    lane = lax.broadcasted_iota(jnp.int32, middle.shape, 1)
    left = jnp.where(lane < 64, beside_column(-1, STRIP), middle)
    right = jnp.where(lane < 64, middle, beside_column(1, 64))
    grid = jnp.concatenate([left, right], axis=1)
    rows = lax.broadcasted_iota(jnp.int32, grid.shape, 0)
    lanes = lax.broadcasted_iota(jnp.int32, grid.shape, 1)
    known = (lanes >= 64 - STRIP) & (lanes < 192 + STRIP)
    rows, lanes = rows + (i - 1) * ROWS, lanes + (j * LANES - 64)
    inside = (rows >= 0) & (rows < gx * ROWS) & (lanes >= 0) & (lanes < gy * LANES) & known
    field = projection(jnp.where(inside, grid, 0.0), inside)
    left, right = pltpu.roll(field[:, 0:128], 64, 1), pltpu.roll(field[:, 128:256], 64, 1)
    lane = lax.broadcasted_iota(jnp.int32, left.shape, 1)
    field_ref[...] = jnp.where(lane < 64, left, right)
    for store in stores:
        store.wait()


def held(x):
    return pltpu.with_memory_space_constraint(x, pltpu.VMEM)


def project(gx, gy, *arrays):
    vmem = pl.BlockSpec(memory_space=pltpu.VMEM)
    hbm = pl.BlockSpec(memory_space=pl.ANY)
    f32 = jnp.float32
    return pl.pallas_call(
        functools.partial(project_kernel, gx, gy),
        name="project",
        out_shape=(
            jax.ShapeDtypeStruct((NS, ROWS, LANES), f32),
            jax.ShapeDtypeStruct((ROWS, LANES), f32),
            jax.ShapeDtypeStruct((ROWS, LANES), f32),
            jax.ShapeDtypeStruct((1, 1), f32),
        ),
        in_specs=[vmem] * len(arrays),
        out_specs=(hbm, hbm, vmem, vmem),
        scratch_shapes=[pltpu.SemaphoreType.DMA((GROUPS + 1,))],
    )(*(held(x) for x in arrays))


def solution(mesh):
    gx, gy = mesh.shape["gx"], mesh.shape["gy"]

    def shards(*args):
        return project(gx, gy, *react(gx, gy, *args))

    return jax.shard_map(
        shards,
        mesh=mesh,
        in_specs=(
            P(None, "gx", "gy"),
            P("gx", "gy"),
            P("gx", "gy"),
            P("gx", "gy"),
            P("gx", "gy"),
            P(),
            P(),
            P(),
            P(),
            P(),
        ),
        out_specs=(P(None, "gx", "gy"), P("gx", "gy"), P("gx", "gy"), P("gx", "gy")),
        check_vma=False,
    )
```

```python
import functools

import jax
import jax.numpy as jnp
from jax import lax
from jax.experimental import pallas as pl
from jax.experimental.pallas import tpu as pltpu
from jax.sharding import PartitionSpec as P

NS = 53
NR = 325
MAXSUB = 4
TILES = 16
ROWS = 32
LANES = 128
STATE = 64
REACT = 336
AHEAD = 2
TEMP_ROW = 53
HEAT_ROW = 54
GROUPS = 4
STRIP = 32
GROUP_ROWS = ROWS // GROUPS
step_time = 0.4
MESH = pl.DeviceIdType.MESH
KEPT = pltpu.VMEM


def halves(x):
    top = x.astype(jnp.bfloat16)
    rest = (x - top.astype(jnp.float32)).astype(jnp.bfloat16)
    return top, rest


SIDES = tuple((a, b) for a in (-1, 0, 1) for b in (-1, 0, 1) if (a, b) != (0, 0))


def shifted(x, by, axis):
    return pltpu.roll(x, by % x.shape[axis], axis)


def beside(u, d):
    return (shifted(u, d, 0) + shifted(u, -d, 0)) + (shifted(u, d, 1) + shifted(u, -d, 1))


def pooled(x, d, row_first, lane_first):
    x = x + jnp.where(row_first, shifted(x, -d, 0), shifted(x, d, 0))
    return x + jnp.where(lane_first, shifted(x, -d, 1), shifted(x, d, 1))


def projection(rhs, inside):
    rows = lax.broadcasted_iota(jnp.int32, rhs.shape, 0)
    lanes = lax.broadcasted_iota(jnp.int32, rhs.shape, 1)
    weigh = jnp.where(inside, 0.2, 0.0)

    def sweep(u, f, d, w):
        return 0.2 * u + w * (f + beside(u, d))

    f0 = rhs
    u0 = sweep(weigh * f0, f0, 1, weigh)
    r0 = f0 - (4.0 * u0 - beside(u0, 1))
    f1 = pooled(r0, 1, (rows & 1) == 0, (lanes & 1) == 0)
    u1 = sweep(weigh * f1, f1, 2, weigh)
    r1 = f1 - (4.0 * u1 - beside(u1, 2))
    f2 = pooled(r1, 2, (rows & 2) == 0, (lanes & 2) == 0)
    u2 = sweep(weigh * f2, f2, 4, weigh)
    u2, f2, w = u2[8:88], f2[8:88], weigh[8:88]
    u2 = sweep(u2, f2, 4, w)
    u2, f2, w = u2[8:72], f2[8:72], weigh[16:80]
    u2 = sweep(u2, f2, 4, w)[8:56]
    middle = slice(24, 72)
    f0, f1, w = f0[middle], f1[middle], weigh[middle]
    u1 = u1[middle] + u2
    for _ in range(2):
        u1 = sweep(u1, f1, 2, w)
    u0 = u0[middle] + u1
    for _ in range(2):
        u0 = sweep(u0, f0, 1, w)
    return u0[8:40]


def peers(gx, gy):
    i = lax.axis_index("gx")
    j = lax.axis_index("gy")

    def there(a, b):
        here = [i + a >= 0] if a < 0 else [i + a < gx] if a > 0 else []
        here += [j + b >= 0] if b < 0 else [j + b < gy] if b > 0 else []
        return functools.reduce(jnp.logical_and, here)

    return i, j, there


def strip(block, start):
    lane = lax.broadcasted_iota(jnp.int32, (8, LANES), 1)
    packed = jnp.zeros((8, LANES), jnp.float32)
    for k in range(GROUPS):
        moved = pltpu.roll(block[8 * k : 8 * k + 8], (STRIP * k - start) % LANES, 1)
        packed = jnp.where((lane >= STRIP * k) & (lane < STRIP * (k + 1)), moved, packed)
    return packed


def react_kernel(
    gx,
    gy,
    counts,
    owners,
    chem_hbm,
    temp_hbm,
    flow_hbm,
    weight_hbm,
    molar_hbm,
    factor_hbm,
    energy_hbm,
    release_hbm,
    out_buf,
    temp_out,
    rhs_ref,
    rows_in,
    strips_in,
    parts,
    chem_buf,
    temp_ref,
    flow_ref,
    weight_ref,
    molar_ref,
    factor_ref,
    energy_ref,
    release_ref,
    state,
    wide,
    energy_cols,
    first,
    second,
    pad,
    widths,
    strips,
    shares,
    in_sem,
    load_sem,
    send,
    recv,
    part_send,
    part_recv,
):
    i, j, there = peers(gx, gy)

    def fetch(g):
        return pltpu.make_async_copy(
            chem_hbm.at[:, pl.ds(g * GROUP_ROWS, GROUP_ROWS), :], chem_buf.at[g], in_sem.at[g]
        )

    loads = [
        pltpu.make_async_copy(source, target, load_sem.at[n])
        for n, (source, target) in enumerate(
            (
                (energy_hbm, energy_ref),
                (factor_hbm, factor_ref),
                (weight_hbm, weight_ref),
                (release_hbm, release_ref),
                (molar_hbm, molar_ref),
                (temp_hbm, temp_ref),
                (flow_hbm, flow_ref),
            )
        )
    ]
    for load in loads[:5]:
        load.start()
    for g in range(GROUPS):
        fetch(g).start()
    for load in loads[5:]:
        load.start()

    pad[...] = jnp.zeros_like(pad)
    wide[...] = jnp.zeros_like(wide)
    state[NS:STATE, :] = jnp.zeros((STATE - NS, ROWS * LANES), jnp.float32)

    turns = lax.broadcasted_iota(jnp.int32, (8, 256), 0)
    for t in range(TILES):
        count = jnp.full((8, 256), counts[0, t], jnp.int32)
        width = step_time / count.astype(jnp.float32)
        widths[:, t * 256 : (t + 1) * 256] = jnp.where(turns < count, width, 0.0)

    barrier = pltpu.get_barrier_semaphore()
    expected = jnp.int32(gx - 1)
    for d in range(1, gx):
        pl.semaphore_signal(
            barrier, inc=1, device_id={"gx": lax.rem(i + d, gx), "gy": j}, device_id_type=MESH
        )
    for a, b in SIDES:
        if b == 0:
            continue
        expected += there(a, b).astype(jnp.int32)

        @pl.when(there(a, b))
        def _(a=a, b=b):
            pl.semaphore_signal(
                barrier, inc=1, device_id={"gx": i + a, "gy": j + b}, device_id_type=MESH
            )

    loads[0].wait()
    pad[0:1, 0:NR] = energy_ref[...].reshape(1, NR) * -1.4426950408889634
    columns = jnp.broadcast_to(pad[...], (LANES, 384)).T[0:REACT]
    energy_cols[:, 0:128] = columns
    energy_cols[:, 128:256] = columns

    loads[1].wait()
    loads[2].wait()
    wide[0:NS, 0:NR] = weight_ref[...] * jnp.exp(factor_ref[...].reshape(1, NR))
    whole = wide[:, 0:384]
    top = whole.astype(jnp.bfloat16).astype(jnp.float32)
    both = jnp.concatenate([top, whole - top], axis=0).T[0:REACT].astype(jnp.bfloat16)
    first[:, 0:128] = both
    first[:, 128:256] = both

    loads[3].wait()
    loads[4].wait()
    wide[0:NS, 0:NR] = molar_ref[...]
    wide[TEMP_ROW : TEMP_ROW + 1, 0:NR] = release_ref[...].reshape(1, NR)
    wide[HEAT_ROW : HEAT_ROW + 1, 0:NR] = release_ref[...].reshape(1, NR)
    whole = wide[0:56, :]
    top = whole.astype(jnp.bfloat16).astype(jnp.float32)
    twice = top + pltpu.roll(top, REACT, 1)
    second[...] = jnp.concatenate([twice, whole - top], axis=0).astype(jnp.bfloat16)

    def take(g):
        fetch(g).wait()
        rows = chem_buf.at[g].reshape(NS * GROUP_ROWS, LANES)
        for r in range(GROUP_ROWS):
            lanes = pl.ds((g * GROUP_ROWS + r) * LANES, LANES)
            state[0:NS, lanes] = rows[pl.ds(r, NS, stride=GROUP_ROWS), :]
            row = g * GROUP_ROWS + r
            state[TEMP_ROW : TEMP_ROW + 1, lanes] = temp_ref[row : row + 1, :]

    def before(step):
        t = step % TILES
        now = state[:, t * 256 : (t + 1) * 256]
        top, rest = halves(now)
        taken = jnp.concatenate([top, top, rest, rest], axis=0)
        return jnp.dot(first[...], taken, preferred_element_type=jnp.float32)

    def middle(step, progress):
        t = step % TILES
        inverse = 1.0 / (1.0 + jnp.abs(state[TEMP_ROW : TEMP_ROW + 1, t * 256 : (t + 1) * 256]))
        flux = jnp.exp2(energy_cols[...] * inverse) * progress
        mixed = jnp.concatenate(halves(flux), axis=0)
        made = jnp.dot(second[:, 0:512], mixed[0:512], preferred_element_type=jnp.float32)
        more = jnp.dot(second[0:64, 512:672], mixed[512:672], preferred_element_type=jnp.float32)
        return made[0:56] + made[56:112] + more[0:56]

    def finish(step, change):
        turn, t = divmod(step, TILES)
        cells = slice(t * 256, (t + 1) * 256)
        state[0:56, cells] += widths[turn : turn + 1, cells] * change

    place = lax.broadcasted_iota(jnp.int32, (TILES, LANES), 0)
    share = jnp.zeros((TILES, LANES), jnp.float32)
    steps = MAXSUB * TILES
    ahead = {}
    loads[5].wait()
    loads[6].wait()
    for step in range(-AHEAD, steps):
        if step + AHEAD < steps:
            group, rest = divmod(step + AHEAD, TILES // GROUPS)
            if group < GROUPS and rest == 0:
                take(group)
            ahead[step + AHEAD] = before(step + AHEAD)
        if step >= 0:
            finish(step, middle(step, ahead.pop(step)))
        if step >= steps - TILES:
            t = step % TILES
            for r in (2 * t, 2 * t + 1):
                heat = state[HEAT_ROW : HEAT_ROW + 1, r * LANES : (r + 1) * LANES]
                rhs_ref[r : r + 1, :] = flow_ref[r : r + 1, :] + heat
                share += jnp.where(place == owners[0, t], heat * heat, 0.0)
    for o in range(TILES):
        shares[o] = share[o : o + 1, :]
    pl.semaphore_wait(barrier, expected)

    def halo(n):
        a, b = SIDES[n]
        slot = len(SIDES) - 1 - n
        return pltpu.make_async_remote_copy(
            src_ref=rhs_ref if b == 0 else strips.at[0 if b < 0 else 1],
            dst_ref=rows_in.at[0 if a > 0 else 1] if b == 0 else strips_in.at[slot],
            send_sem=send.at[n],
            recv_sem=recv.at[slot],
            device_id={"gx": i + a, "gy": j + b},
            device_id_type=MESH,
        )

    def part(d):
        peer = lax.rem(i + d, gx)
        return pltpu.make_async_remote_copy(
            src_ref=shares.at[peer],
            dst_ref=parts.at[d],
            send_sem=part_send,
            recv_sem=part_recv,
            device_id={"gx": peer, "gy": j},
            device_id_type=MESH,
        )

    def send_to(*order):
        for n in order:

            @pl.when(there(*SIDES[n]))
            def _(n=n):
                halo(n).start()

    send_to(1, 6)
    for d in range(1, gx):
        part(d).start()
    block = rhs_ref[...]
    strips[0] = strip(block, 0)
    strips[1] = strip(block, LANES - STRIP)
    send_to(0, 2, 5, 7, 3, 4)

    parts[0] = shares[i]
    for r in range(ROWS):
        temp_out[r : r + 1, :] = state[TEMP_ROW : TEMP_ROW + 1, r * LANES : (r + 1) * LANES]
    for g in range(GROUPS):
        rows = out_buf.at[g].reshape(NS * GROUP_ROWS, LANES)
        for r in range(GROUP_ROWS):
            lanes = pl.ds((g * GROUP_ROWS + r) * LANES, LANES)
            rows[pl.ds(r, NS, stride=GROUP_ROWS), :] = state[0:NS, lanes]

    for n in range(len(SIDES)):
        @pl.when(there(*SIDES[n]))
        def _(n=n):
            halo(len(SIDES) - 1 - n).wait_recv()

    pltpu.make_async_copy(parts.at[pl.ds(1, gx - 1)], parts.at[pl.ds(1, gx - 1)], part_recv).wait()

    for n in range(len(SIDES)):

        @pl.when(there(*SIDES[n]))
        def _(n=n):
            halo(n).wait_send()

    pltpu.make_async_copy(shares.at[pl.ds(1, gx - 1)], shares.at[pl.ds(1, gx - 1)], part_send).wait()


def react(gx, gy, chem, temp, flow, counts, owners, weight, molar, factor, energy, release):
    vmem = pl.BlockSpec(memory_space=pltpu.VMEM)
    smem = pl.BlockSpec(memory_space=pltpu.SMEM)
    hbm = pl.BlockSpec(memory_space=pl.ANY)
    f32 = jnp.float32
    sides = len(SIDES)
    dma = pltpu.SemaphoreType.DMA
    return pl.pallas_call(
        functools.partial(react_kernel, gx, gy),
        name="react",
        out_shape=(
            KEPT((GROUPS, NS, GROUP_ROWS, LANES), f32),
            KEPT((ROWS, LANES), f32),
            KEPT((ROWS, LANES), f32),
            KEPT((2, ROWS, LANES), f32),
            KEPT((sides, 8, LANES), f32),
            KEPT((gx, 1, LANES), f32),
        ),
        in_specs=[smem, smem] + [hbm] * 8,
        out_specs=(vmem,) * 6,
        scratch_shapes=[
            pltpu.VMEM((GROUPS, NS, GROUP_ROWS, LANES), f32),
            pltpu.VMEM((ROWS, LANES), f32),
            pltpu.VMEM((ROWS, LANES), f32),
            pltpu.VMEM((NS, NR), f32),
            pltpu.VMEM((NS, NR), f32),
            pltpu.VMEM((NR,), f32),
            pltpu.VMEM((NR,), f32),
            pltpu.VMEM((NR,), f32),
            pltpu.VMEM((STATE, ROWS * LANES), f32),
            pltpu.VMEM((STATE, 768), f32),
            pltpu.VMEM((REACT, 256), f32),
            pltpu.VMEM((REACT, 256), jnp.bfloat16),
            pltpu.VMEM((112, 768), jnp.bfloat16),
            pltpu.VMEM((1, 384), f32),
            pltpu.VMEM((8, ROWS * LANES), f32),
            pltpu.VMEM((2, 8, LANES), f32),
            pltpu.VMEM((TILES, 1, LANES), f32),
            dma((GROUPS,)),
            dma((7,)),
            dma((sides,)),
            dma((sides,)),
            dma(()),
            dma(()),
        ],
        compiler_params=pltpu.CompilerParams(collective_id=0, has_side_effects=True),
    )(counts, owners, chem, temp, flow, weight.T, molar.T, factor, energy, release)


def project_kernel(
    gx,
    gy,
    chem_ref,
    temp_ref,
    rhs_ref,
    rows_in,
    strips_in,
    parts,
    chem_out,
    temp_out,
    field_ref,
    burden_ref,
    sem,
):
    i, j, _ = peers(gx, gy)
    stores = [
        pltpu.make_async_copy(
            chem_ref.at[g], chem_out.at[:, pl.ds(g * GROUP_ROWS, GROUP_ROWS), :], sem.at[g]
        )
        for g in range(GROUPS)
    ]
    stores.append(pltpu.make_async_copy(temp_ref, temp_out, sem.at[GROUPS]))
    for store in stores:
        store.start()

    total = parts[0]
    for d in range(1, gx):
        total = total + parts[d]
    burden_ref[...] = jnp.sum(total, axis=1, keepdims=True) / float(ROWS * LANES)

    middle = jnp.concatenate([rows_in[0], rhs_ref[...], rows_in[1]], axis=0)
    middle = pltpu.roll(middle, 64, 1)

    def beside_column(b, at):
        column = []
        for a in (-1, 0, 1):
            packed = strips_in[SIDES.index((a, b))]
            column += [pltpu.roll(packed, (at - STRIP * k) % LANES, 1) for k in range(GROUPS)]
        return jnp.concatenate(column, axis=0)

    lane = lax.broadcasted_iota(jnp.int32, middle.shape, 1)
    left = jnp.where(lane < 64, beside_column(-1, STRIP), middle)
    right = jnp.where(lane < 64, middle, beside_column(1, 64))
    grid = jnp.concatenate([left, right], axis=1)
    rows = lax.broadcasted_iota(jnp.int32, grid.shape, 0)
    lanes = lax.broadcasted_iota(jnp.int32, grid.shape, 1)
    known = (lanes >= 64 - STRIP) & (lanes < 192 + STRIP)
    rows, lanes = rows + (i - 1) * ROWS, lanes + (j * LANES - 64)
    inside = (rows >= 0) & (rows < gx * ROWS) & (lanes >= 0) & (lanes < gy * LANES) & known
    field = projection(jnp.where(inside, grid, 0.0), inside)
    left, right = pltpu.roll(field[:, 0:128], 64, 1), pltpu.roll(field[:, 128:256], 64, 1)
    lane = lax.broadcasted_iota(jnp.int32, left.shape, 1)
    field_ref[...] = jnp.where(lane < 64, left, right)
    for store in stores:
        store.wait()


def held(x):
    return pltpu.with_memory_space_constraint(x, pltpu.VMEM)


def project(gx, gy, *arrays):
    vmem = pl.BlockSpec(memory_space=pltpu.VMEM)
    hbm = pl.BlockSpec(memory_space=pl.ANY)
    f32 = jnp.float32
    return pl.pallas_call(
        functools.partial(project_kernel, gx, gy),
        name="project",
        out_shape=(
            jax.ShapeDtypeStruct((NS, ROWS, LANES), f32),
            jax.ShapeDtypeStruct((ROWS, LANES), f32),
            jax.ShapeDtypeStruct((ROWS, LANES), f32),
            jax.ShapeDtypeStruct((1, 1), f32),
        ),
        in_specs=[vmem] * len(arrays),
        out_specs=(hbm, hbm, vmem, vmem),
        scratch_shapes=[pltpu.SemaphoreType.DMA((GROUPS + 1,))],
    )(*(held(x) for x in arrays))


def solution(mesh):
    gx, gy = mesh.shape["gx"], mesh.shape["gy"]

    def shards(*args):
        return project(gx, gy, *react(gx, gy, *args))

    return jax.shard_map(
        shards,
        mesh=mesh,
        in_specs=(
            P(None, "gx", "gy"),
            P("gx", "gy"),
            P("gx", "gy"),
            P("gx", "gy"),
            P("gx", "gy"),
            P(),
            P(),
            P(),
            P(),
            P(),
        ),
        out_specs=(P(None, "gx", "gy"), P("gx", "gy"), P("gx", "gy"), P("gx", "gy")),
        check_vma=False,
    )
```
